32 devices in a mesh: dom: 8 (over z, y), col: 2 (over x), batch: 2 (over core).
Axes of the slice: x: 2, y: 2, z: 4, core: 2. Of those that a mesh axis runs over, the one named last changes fastest.
Arguments:
- features: bfloat16 [16384, 128], P('dom', 'col'), may hold values from -6 to 6
- self_weight1: bfloat16 [128, 256], P('col', 'batch'), may hold values from -0.5 to 0.5
- neigh_weight1: bfloat16 [128, 256], P('col', 'batch'), may hold values from -2 to 2
- need_first: int32 [16, 64], P(('dom', 'batch')), may hold values from 0 to 127, as said below
- count_first: int32 [16], P(('dom', 'batch')), may hold values from 0 to 64
- adjacency_first: int32 [16384, 512], P(('dom', 'batch')), may hold values from 0 to 16384, as said below
- self_weight2: bfloat16 [256, 172], P('col', 'batch'), may hold values from -0.375 to 0.375
- neigh_weight2: bfloat16 [256, 172], P('col', 'batch'), may hold values from -0.375 to 0.375
- need_second: int32 [16, 64], P(('dom', 'batch')), may hold values from 0 to 127, as said below
- count_second: int32 [16], P(('dom', 'batch')), may hold values from 0 to 64
- adjacency_second: int32 [16384, 512], P(('dom', 'batch')), may hold values from 0 to 16384, as said below
- seed_rows: int32 [16384], P(('dom', 'batch')), may hold values from 0 to 2047
Outputs:
- logits: float32 [16384, 172], P(('dom', 'batch'))
The draws below stay inside these ranges and needn't reach their ends.
Inputs may be any that keep to these rules, and one draw needn't show every extreme that they name: `need_first`: each row lists 64 different node blocks in increasing order; block g holds nodes 128 * g to 128 * g + 127 and lies in partition g // 16. At most 16 entries of one row lie in one partition, and exactly 16 lie in some partition in every row. `need_second`: each row lists 64 different frontier blocks in increasing order; block g holds frontier rows 128 * g to 128 * g + 127 and lies in partition g // 16. At most 16 entries of one row lie in one partition, and exactly 16 lie in some partition in every row. `adjacency_first`: bit i of word k of a row is the adjacency entry of column 16 k + i; at most one bit of a word is set, and bit 15 never. `adjacency_second`: bit i of word k of a row is the adjacency entry of column 16 k + i; at most one bit of a word is set, and bit 15 never.
All inputs are finite; a program needn't handle non-finite values.
Results may differ from the reference program's by a relative error of at most 0.0036.
Values may be sent and summed in bfloat16 or wider, within the bound.
No kernel may reach another device: no remote copies, remote signals or barrier semaphores. Data moves between devices by JAX's collectives and lax.ppermute only.
A program may use at most 128 MiB of HBM per device.

```python
import math
import jax
import jax.numpy as jnp
from jax import lax

F = 128
HID = 256
CLASSES = 172
BLK = 128
NB_DEV = 16
T1_DEV = 1024
SEED_DEV = 1024
NEED1 = 64
NEED2 = 64
NODE_DEV = 2048
NODES = 16384
SEEDS = 16384
N_DOM = 8
N_BATCH = 2


def block_lists(key, rows, need_len, owners, owned):
    capacity = max(2, (2 * need_len + owners - 1) // owners)

    def one_row(row_key):
        key_list = jax.random.split(row_key, 4)
        boost_by = jax.random.randint(key_list[0], (owners,), 0, 4) * 2 ** 20
        leader = jax.random.randint(key_list[1], (), 0, owners)
        boost_by = jnp.where(jnp.arange(owners) == leader, 8 * 2 ** 20, boost_by)
        candidate_owner = jnp.arange(owners * capacity) // capacity
        scores = boost_by[candidate_owner] + jax.random.randint(key_list[2], (owners * capacity,), 0, 2 ** 20)
        ranking = jnp.argsort(-scores, stable=True)
        picked = ranking[:need_len]
        picked_owner = picked // capacity
        picked_rank = picked % capacity
        shuffle_scores = jax.random.randint(key_list[3], (owners, owned), 0, 2 ** 20)
        shuffles = jnp.argsort(shuffle_scores, axis=1, stable=True)
        local_block = shuffles[picked_owner, picked_rank]
        return jnp.sort(picked_owner * owned + local_block).astype(jnp.int32)
    return jax.vmap(one_row)(jax.random.split(key, rows))


def packed_adjacency(key, rows, width, columns):
    spread = max(16, columns // 24)
    drawn = jax.random.randint(key, (rows, width), 0, spread)
    single = jnp.left_shift(jnp.ones_like(drawn), jnp.minimum(drawn, 14))
    return jnp.where(drawn < 15, single, 0).astype(jnp.int32)


def draw_need_first(key, part):
    return block_lists(jax.random.fold_in(key, 11), N_DOM * N_BATCH, NEED1, N_DOM, NB_DEV)


def draw_need_second(key, part):
    return block_lists(jax.random.fold_in(key, 23), N_DOM * N_BATCH, NEED2, N_DOM, N_BATCH * T1_DEV // BLK)


def draw_adjacency_first(key, part):
    return packed_adjacency(jax.random.fold_in(key, 37), N_DOM * N_BATCH * T1_DEV, NEED1 * BLK // 16, NEED1 * BLK)


def draw_adjacency_second(key, part):
    return packed_adjacency(jax.random.fold_in(key, 41), N_DOM * N_BATCH * SEED_DEV, NEED2 * BLK // 16, NEED2 * BLK)


def touch_ends(values, rng, least, largest):
    longest = values.shape.index(max(values.shape))
    spots = []
    for shift in (0, 1):
        where = [jax.random.randint(jax.random.fold_in(rng, axis), (), 0, length) for axis, length in enumerate(values.shape)]
        where[longest] = (where[longest] + shift) % values.shape[longest]
        spots.append(tuple(where))
    return values.at[spots[0]].set(least).at[spots[1]].set(largest)


def block_scale(stream_key, shape, pieces, least, high):
    def one(axis_at, shards_of):
        heights = jax.random.uniform(jax.random.fold_in(jax.random.fold_in(stream_key, 6), axis_at), (shards_of,), jnp.float32, least / len(pieces), high / len(pieces))
        return jnp.repeat(jnp.exp(heights), shape[axis_at] // shards_of).reshape((-1,) + (1,) * (len(shape) - axis_at - 1))

    factor_of = one(*pieces[0])
    for cut in pieces[1:]:
        factor_of = factor_of * one(*cut)
    return factor_of


def gaussian(key, dims, scale, bound, pieces=(), held_as=jnp.bfloat16):
    values = scale * jax.random.normal(key, dims, jnp.float32)
    if pieces:
        values = values * block_scale(key, dims, pieces, -0.22, 0.18)
    return jnp.clip(values, -bound, bound).astype(held_as)


def setup_inputs(seed: int = 0) -> dict:
    arg_keys = jax.random.split(jax.random.key(seed), 13)
    features = gaussian(arg_keys[0], (NODES, F), 1.0, 6.0, ((0, 8), (1, 2)))
    self_weight1 = gaussian(arg_keys[1], (F, HID), F ** -0.5, 0.5, ((0, 2), (1, 2)))
    neigh_weight1 = gaussian(arg_keys[2], (F, HID), (F // 16) ** -0.5, 2.0, ((0, 2), (1, 2)))
    need_first = draw_need_first(jax.random.fold_in(arg_keys[12], 71), 0)
    count_first = touch_ends(jax.random.randint(arg_keys[4], (N_DOM * N_BATCH,), 0, NEED1 + 1), jax.random.fold_in(arg_keys[4], 1), 0, NEED1).astype(jnp.int32)
    adjacency_first = draw_adjacency_first(jax.random.fold_in(arg_keys[12], 71), 0)
    self_weight2 = gaussian(arg_keys[6], (HID, CLASSES), HID ** -0.5, 0.375, ((0, 2), (1, 2)))
    neigh_weight2 = gaussian(arg_keys[7], (HID, CLASSES), HID ** -0.5, 0.375, ((0, 2), (1, 2)))
    need_second = draw_need_second(jax.random.fold_in(arg_keys[12], 71), 0)
    count_second = touch_ends(jax.random.randint(arg_keys[9], (N_DOM * N_BATCH,), 0, NEED2 + 1), jax.random.fold_in(arg_keys[9], 1), 0, NEED2).astype(jnp.int32)
    adjacency_second = draw_adjacency_second(jax.random.fold_in(arg_keys[12], 71), 0)
    seed_rows = touch_ends(jax.random.randint(arg_keys[11], (SEEDS,), 0, N_BATCH * T1_DEV), jax.random.fold_in(arg_keys[11], 1), 0, (N_BATCH * T1_DEV) - 1).astype(jnp.int32)
    return {"features": features, "self_weight1": self_weight1, "neigh_weight1": neigh_weight1, "need_first": need_first, "count_first": count_first, "adjacency_first": adjacency_first, "self_weight2": self_weight2, "neigh_weight2": neigh_weight2, "need_second": need_second, "count_second": count_second, "adjacency_second": adjacency_second, "seed_rows": seed_rows}


def unpack_rows(packed_rows, valid_cols):
    shifts = jnp.arange(16, dtype=jnp.int32)
    bit_table = jnp.right_shift(packed_rows[:, :, None], shifts[None, None, :]) & 1
    bit_table = bit_table.reshape(packed_rows.shape[0], packed_rows.shape[1] * 16)
    column = jnp.arange(bit_table.shape[1], dtype=jnp.int32)
    return jnp.where(column[None, :] < valid_cols, bit_table, 0)


def mean_rows(packed, valid_cols, needed):
    total_rows = packed.shape[0]
    row_block = math.gcd(total_rows, 256)
    grouped = packed.reshape(total_rows // row_block, row_block, packed.shape[1])

    def one_block(row_piece):
        dense_rows = unpack_rows(row_piece, valid_cols)
        degree = jnp.sum(dense_rows, axis=1).astype(jnp.float32)
        summed = jnp.dot(dense_rows.astype(jnp.bfloat16), needed, preferred_element_type=jnp.float32)
        return (summed / jnp.maximum(degree, 1.0)[:, None]).astype(jnp.bfloat16)

    return lax.map(one_block, grouped).reshape(total_rows, needed.shape[1])


def layer_means(packed_all, counts, lists, blocks, rows_dev):
    workers = counts.shape[0]
    width = blocks.shape[1] // BLK

    def per_worker(worker):
        packed = lax.dynamic_slice_in_dim(packed_all, worker * rows_dev, rows_dev, 0)
        chosen = jnp.take(blocks, lists[worker], axis=0)
        needed = chosen.reshape(chosen.shape[0] * BLK, width)
        return mean_rows(packed, counts[worker] * BLK, needed)

    return lax.map(per_worker, jnp.arange(workers, dtype=jnp.int32)).reshape(workers * rows_dev, width)


def reference(features, self_weight1, neigh_weight1, need_first, count_first, adjacency_first, self_weight2, neigh_weight2, need_second, count_second, adjacency_second, seed_rows):
    workers = N_DOM * N_BATCH
    node_blocks = features.reshape(N_DOM * NB_DEV, BLK * F)
    near_first = layer_means(adjacency_first, count_first, need_first, node_blocks, T1_DEV)
    worker_ids = jnp.arange(workers, dtype=jnp.int32)
    starts = (worker_ids // N_BATCH) * NODE_DEV + (worker_ids % N_BATCH) * T1_DEV
    self_first = lax.map(lambda row_start: lax.dynamic_slice_in_dim(features, row_start, T1_DEV, 0), starts)
    self_first = self_first.reshape(workers * T1_DEV, F)
    pre_first = jnp.dot(self_first, self_weight1, preferred_element_type=jnp.float32) + jnp.dot(near_first, neigh_weight1, preferred_element_type=jnp.float32)
    hidden_first = jnp.maximum(pre_first, 0.0).astype(jnp.bfloat16)
    front_blocks = hidden_first.reshape(workers * T1_DEV // BLK, BLK * HID)
    near_second = layer_means(adjacency_second, count_second, need_second, front_blocks, SEED_DEV)
    seed_owner = jnp.arange(workers * SEED_DEV, dtype=jnp.int32) // SEED_DEV
    own_rows = (seed_owner // N_BATCH) * (N_BATCH * T1_DEV) + seed_rows
    own_second = jnp.take(hidden_first, own_rows, axis=0)
    logits = jnp.dot(own_second, self_weight2, preferred_element_type=jnp.float32) + jnp.dot(near_second, neigh_weight2, preferred_element_type=jnp.float32)
    return logits
```

```python
import functools

import jax
import jax.numpy as jnp
from jax import lax
from jax.experimental import pallas as pl
from jax.experimental.pallas import tpu as pltpu
from jax.sharding import PartitionSpec as P

BLK = 128
BITS = 16
PLANES = 15
WORDS = BLK // BITS
LANES = 128
MESH_AXES = ("dom", "col", "batch")
VMEM = pl.BlockSpec(memory_space=pltpu.VMEM)
SMEM = pl.BlockSpec(memory_space=pltpu.SMEM)
ANY = pl.BlockSpec(memory_space=pl.ANY)


def lanes_for(width):
    need = max((PLANES - 1) * width + LANES, BITS * width if width % 64 == 0 else 0)
    return -(-need // LANES) * LANES


def shift_perm(sizes, which, by):
    pairs = []
    total = 1
    for size in sizes:
        total *= size
    for source in range(total):
        place = []
        rest = source
        for size in reversed(sizes):
            place.append(rest % size)
            rest //= size
        place = place[::-1]
        place[which] = (place[which] + by) % sizes[which]
        target = 0
        for size, at in zip(sizes, place):
            target = target * size + at
        pairs.append((source, target))
    return pairs


def pack_planes(tall_ref, out_ref, width, planes):
    words = out_ref.shape[0]
    for i in range(planes):
        piece = tall_ref[pl.ds(i, words, stride=BITS), :]
        out_ref[:, i * width : (i + 1) * width] = piece[:, :width]


def sums_of_tile(adj_ref, count, table_ref):
    words = adj_ref[...]
    column = lax.broadcasted_iota(jnp.int32, words.shape, 1)
    words = jnp.where(column < count * WORDS, words, 0)
    degree = jnp.sum(jnp.where(words != 0, 1.0, 0.0), axis=1, keepdims=True)
    mask = jnp.concatenate(
        [jnp.where(words == (1 << i), 1.0, 0.0).astype(jnp.bfloat16) for i in range(PLANES)], axis=1
    )
    summed = jnp.dot(mask, table_ref[...], preferred_element_type=jnp.float32)
    return summed / jnp.maximum(degree, 1.0)


def build_table(src_ref, pieces, stack_ref, picked_ref, table_ref, sem, width):
    blocks = pieces[0].shape[0]
    copies = [
        pltpu.make_async_copy(piece, stack_ref.at[pl.ds(n * blocks, blocks)], sem.at[n])
        for n, piece in enumerate(pieces)
    ]
    for copy in copies:
        copy.start()
    for copy in copies:
        copy.wait()
    listed = src_ref.shape[0]

    def pick(b, _):
        picked_ref[pl.ds(pl.multiple_of(b * WORDS, WORDS), WORDS), :] = stack_ref[src_ref[b]].astype(jnp.float32)
        return 0

    lax.fori_loop(0, listed, pick, 0, unroll=8)
    rows = listed * WORDS
    for i in range(PLANES):
        table_ref[pl.ds(i * rows, rows), :] = picked_ref[:, i * width : i * width + LANES].astype(jnp.bfloat16)


def mean_first_kernel(width, n_pieces, src_ref, count_ref, adj_ref, *rest):
    pieces, out_ref = rest[:n_pieces], rest[n_pieces]
    stack_ref, picked_ref, table_ref, tall_ref, wide_ref, sem = rest[n_pieces + 1 :]

    @pl.when(pl.program_id(0) == 0)
    def _():
        build_table(src_ref, pieces, stack_ref, picked_ref, table_ref, sem, width)

    tall_ref[...] = sums_of_tile(adj_ref, count_ref[0], table_ref)
    pack_planes(tall_ref, wide_ref, width, BITS)
    out_ref[...] = wide_ref[...].astype(jnp.bfloat16)


def mean_second_kernel(width, n_pieces, src_ref, count_ref, adj_ref, own_ref, *rest):
    pieces, out_ref = rest[:n_pieces], rest[n_pieces]
    stack_ref, picked_ref, table_ref, sem = rest[n_pieces + 1 :]

    @pl.when(pl.program_id(0) == 0)
    def _():
        build_table(src_ref, pieces, stack_ref, picked_ref, table_ref, sem, width)

    mean = sums_of_tile(adj_ref, count_ref[0], table_ref)
    out_ref[...] = (mean.T[:width, :] + own_ref[...]).astype(jnp.bfloat16)


def mean_call(kernel, src, count, adjacency, own, pieces, out_shape, out_block, extra, name, width):
    rows, row_words = adjacency.shape
    tile = rows // 4 if rows % 64 == 0 else rows
    blocks, words, lanes = pieces[0].shape
    listed = src.shape[0]
    in_specs = [SMEM, SMEM, pl.BlockSpec((tile, row_words), lambda r: (r, 0))]
    args = [src, count, adjacency]
    if own is not None:
        in_specs.append(pl.BlockSpec((own.shape[0], tile), lambda r: (0, r)))
        args.append(own)
    return pl.pallas_call(
        functools.partial(kernel, width, len(pieces)),
        grid=(rows // tile,),
        in_specs=in_specs + [ANY] * len(pieces),
        out_specs=out_block(tile),
        out_shape=out_shape,
        scratch_shapes=[
            pltpu.VMEM((len(pieces) * blocks, words, lanes), jnp.bfloat16),
            pltpu.VMEM((listed * words, lanes), jnp.float32),
            pltpu.VMEM((PLANES * listed * words, LANES), jnp.bfloat16),
        ]
        + extra(tile)
        + [pltpu.SemaphoreType.DMA((len(pieces),))],
        compiler_params=pltpu.CompilerParams(dimension_semantics=("arbitrary",)),
        name=name,
    )(*args, *pieces)


def hidden_kernel(width, classes, self_own, self_far, near_own, near_far, weight_ref, out_weight_ref, hidden_ref, wide_ref, rows_ref, tall_ref, scratch_ref):
    words = self_own.shape[0]
    parts = (self_own, self_far, near_own, near_far)
    for i in range(BITS):
        for n, part in enumerate(parts):
            rows_ref[pl.ds(i * words, words), n * width : (n + 1) * width] = part[:, i * width : (i + 1) * width]
    hidden = jnp.dot(rows_ref[...], weight_ref[...], preferred_element_type=jnp.float32)
    hidden = jnp.maximum(hidden, 0.0).astype(jnp.bfloat16)
    hidden_ref[...] = hidden
    tall_ref[...] = jnp.dot(hidden, out_weight_ref[...], preferred_element_type=jnp.float32)
    scratch_ref[...] = jnp.zeros_like(scratch_ref)
    for i in range(PLANES):
        scratch_ref[:, i * classes : (i + 1) * classes] = tall_ref[pl.ds(i * words, words), :classes]
    wide_ref[...] = scratch_ref[...].astype(jnp.bfloat16)


def own_kernel(seed_ref, weight_ref, *rest):
    hidden_refs, out_ref = rest[:-1], rest[-1]
    total = jnp.zeros(out_ref.shape, jnp.float32)
    for n, hidden_ref in enumerate(hidden_refs):
        rows = hidden_ref.shape[0]
        every = lax.dot_general(
            weight_ref[...], hidden_ref[...], (((1,), (1,)), ((), ())), preferred_element_type=jnp.float32
        )
        high = every.astype(jnp.bfloat16)
        low = (every - high.astype(jnp.float32)).astype(jnp.bfloat16)
        place = lax.broadcasted_iota(jnp.int32, (rows, seed_ref.shape[1]), 0) + n * rows
        chosen = jnp.where(place == seed_ref[...], 1.0, 0.0).astype(jnp.bfloat16)
        total += jnp.dot(high, chosen, preferred_element_type=jnp.float32)
        total += jnp.dot(low, chosen, preferred_element_type=jnp.float32)
    out_ref[...] = total


def per_device(
    sizes,
    features,
    self_weight1,
    neigh_weight1,
    need_first,
    count_first,
    adjacency_first,
    self_weight2,
    neigh_weight2,
    need_second,
    count_second,
    adjacency_second,
    seed_rows,
):
    n_dom, n_col, n_batch = sizes
    inner = 2 if n_dom % 2 == 0 else 1
    outer = n_dom // inner
    grid = (outer, inner, n_col, n_batch)
    dom_at, col_at, batch_at = (lax.axis_index(a) for a in MESH_AXES)

    def move(array, which, by):
        return lax.ppermute(array, MESH_AXES, shift_perm(grid, which, by))

    def ring(array, which):
        return [array] + [move(array, which, by) for by in range(1, grid[which])]

    def gather_blocks(piece):
        return [
            last for first in ring(piece, 0) for second in ring(first, 1) for last in ring(second, 3)
        ]

    def in_order(relative, at):
        n = len(relative)
        ordered = []
        for owner in range(n):
            chosen = relative[0]
            for back in range(1, n):
                chosen = jnp.where((at - owner) % n == back, relative[back], chosen)
            ordered.append(chosen)
        return ordered

    width = features.shape[1]
    rows = adjacency_first.shape[0]
    words = rows // BITS
    lanes = lanes_for(width)
    blocks = rows // BLK
    part_blocks = blocks * n_batch

    def sources(wanted):
        owner, local = wanted // part_blocks, wanted % part_blocks
        back_outer = (dom_at // inner - owner // inner) % outer
        back_inner = (dom_at - owner) % inner
        back_batch = (batch_at - local // blocks) % n_batch
        return ((back_outer * inner + back_inner) * n_batch + back_batch) * blocks + local % blocks

    own = lax.dynamic_slice_in_dim(features, batch_at * rows, rows, 0).reshape(words, BITS * width)
    if lanes > BITS * width:
        own = jnp.pad(own, ((0, 0), (0, lanes - BITS * width)))
    pieces_first = gather_blocks(own.reshape(blocks, WORDS, lanes))

    self_parts = ring(own, 2)
    class_cols = self_weight2.shape[1]
    hidden_rows = self_weight2.shape[0]
    packed = jnp.concatenate([self_weight1, neigh_weight1], axis=0)
    packed2 = jnp.concatenate([self_weight2.T, neigh_weight2.T], axis=0)
    packs = [ring(a, 3) for a in ring(packed, 2)]
    packs2 = [ring(a, 3) for a in ring(packed2, 2)]
    full = [jnp.concatenate(in_order(row, batch_at), axis=1) for row in packs]
    weight_first = jnp.concatenate([f[:width] for f in full] + [f[width:] for f in full], axis=0)
    rows2 = [in_order(row, batch_at) for row in packs2]
    classes = class_cols * n_batch // n_col

    def class_rows(low):
        whole = jnp.concatenate(
            in_order([jnp.concatenate([a[low : low + class_cols] for a in row], axis=0) for row in rows2], col_at),
            axis=1,
        )
        return lax.dynamic_slice_in_dim(whole, col_at * classes, classes, 0)

    weight_own = class_rows(0)
    weight_far = jnp.pad(class_rows(class_cols).T, ((0, 0), (0, LANES - classes)))

    near = mean_call(
        mean_first_kernel,
        sources(need_first[0]),
        count_first,
        adjacency_first,
        None,
        pieces_first,
        jax.ShapeDtypeStruct((words, lanes), jnp.bfloat16),
        lambda tile: pl.BlockSpec((tile // BITS, lanes), lambda r: (r, 0)),
        lambda tile: [pltpu.VMEM((tile, LANES), jnp.float32), pltpu.VMEM((tile // BITS, lanes), jnp.float32)],
        "mean_first",
        width,
    )
    near_parts = ring(near, 2)
    wide = lanes_for(classes)
    hidden, scores = pl.pallas_call(
        functools.partial(hidden_kernel, width, classes),
        in_specs=[VMEM] * 6,
        out_specs=[VMEM] * 2,
        out_shape=[
            jax.ShapeDtypeStruct((rows, weight_first.shape[1]), jnp.bfloat16),
            jax.ShapeDtypeStruct((words, wide), jnp.bfloat16),
        ],
        scratch_shapes=[
            pltpu.VMEM((rows, weight_first.shape[0]), jnp.bfloat16),
            pltpu.VMEM((rows, LANES), jnp.float32),
            pltpu.VMEM((words, wide), jnp.float32),
        ],
        name="hidden",
    )(*self_parts, *near_parts, weight_first, weight_far)

    pieces_second = gather_blocks(scores.reshape(blocks, WORDS, wide))
    inside = seed_rows % rows
    place = ((batch_at - seed_rows // rows) % n_batch) * rows + (inside % BITS) * words + inside // BITS
    seeds = seed_rows.shape[0]
    own_second = pl.pallas_call(
        own_kernel,
        in_specs=[VMEM] * (2 + n_batch),
        out_specs=VMEM,
        out_shape=jax.ShapeDtypeStruct((classes, seeds), jnp.float32),
        name="own_rows",
    )(place.reshape(1, seeds), weight_own, *ring(hidden, 3))
    half = mean_call(
        mean_second_kernel,
        sources(need_second[0]),
        count_second,
        adjacency_second,
        own_second,
        pieces_second,
        jax.ShapeDtypeStruct((classes, seeds), jnp.bfloat16),
        lambda tile: pl.BlockSpec((classes, tile), lambda r: (0, r)),
        lambda tile: [],
        "mean_second",
        classes,
    )
    logits = jnp.concatenate(in_order(ring(half, 2), col_at), axis=0)
    return logits.astype(jnp.float32).T


def solution(mesh):
    sizes = tuple(mesh.shape[a] for a in MESH_AXES)
    placed = (
        P("dom", "col"),
        P("col", "batch"),
        P("col", "batch"),
        P(("dom", "batch"), None),
        P(("dom", "batch")),
        P(("dom", "batch"), None),
        P("col", "batch"),
        P("col", "batch"),
        P(("dom", "batch"), None),
        P(("dom", "batch")),
        P(("dom", "batch"), None),
        P(("dom", "batch")),
    )
    return jax.shard_map(
        functools.partial(per_device, sizes),
        mesh=mesh,
        in_specs=placed,
        out_specs=P(("dom", "batch"), None),
        check_vma=False,
    )
```

```python
import functools

import jax
import jax.numpy as jnp
from jax import lax
from jax.experimental import pallas as pl
from jax.experimental.pallas import tpu as pltpu
from jax.sharding import PartitionSpec as P


BLK = 128
BITS = 16
PLANES = 15
WORDS = BLK // BITS
LANES = 128
MESH_AXES = ("dom", "col", "batch")
VMEM = pl.BlockSpec(memory_space=pltpu.VMEM)
SMEM = pl.BlockSpec(memory_space=pltpu.SMEM)
ANY = pl.BlockSpec(memory_space=pl.ANY)
PARAMS = pltpu.CompilerParams(vmem_limit_bytes=36 * 2**20)


def lanes_for(width):
    need = max((PLANES - 1) * width + LANES, BITS * width if width % 64 == 0 else 0)
    return -(-need // LANES) * LANES


def shift_perm(sizes, which, by):
    pairs = []
    total = 1
    for size in sizes:
        total *= size
    for source in range(total):
        place = []
        rest = source
        for size in reversed(sizes):
            place.append(rest % size)
            rest //= size
        place = place[::-1]
        place[which] = (place[which] + by) % sizes[which]
        target = 0
        for size, at in zip(sizes, place):
            target = target * size + at
        pairs.append((source, target))
    return pairs


def pack_planes(tall_ref, out_ref, width, planes):
    words = out_ref.shape[0]
    for i in range(planes):
        piece = tall_ref[pl.ds(i, words, stride=BITS), :]
        out_ref[:, i * width : (i + 1) * width] = piece[:, :width]


def fetch_words(adj_ref, words_ref, sem):
    rows = adj_ref.shape[0] // sem.shape[0]
    copies = [
        pltpu.make_async_copy(adj_ref.at[pl.ds(n * rows, rows)], words_ref.at[pl.ds(n * rows, rows)], sem.at[n])
        for n in range(sem.shape[0])
    ]
    for copy in copies:
        copy.start()
    return copies


def pick_blocks(low_ref, high_ref, local_ref, pieces, picked_ref):
    for n, piece in enumerate(pieces):

        def pick(b, _, piece=piece):
            at = pl.multiple_of(b * WORDS, WORDS)
            picked_ref[pl.ds(at, WORDS), :] = piece[local_ref[b]].astype(jnp.float32)
            return 0

        lax.fori_loop(low_ref[n], high_ref[n], pick, 0)


def mean_rows(count, words_ref, copies, short_ref, picked_ref, total_ref, width):
    rows = words_ref.shape[0] // len(copies)
    degrees = []
    for n, copy in enumerate(copies):
        copy.wait()
        words = words_ref[n * rows : (n + 1) * rows, :]
        column = lax.broadcasted_iota(jnp.int32, words.shape, 1)
        words = jnp.where(column < count * WORDS, words, 0)
        degrees.append(jnp.sum(jnp.where(words != 0, 1.0, 0.0), axis=1, keepdims=True))
        short_ref[n * rows : (n + 1) * rows, :] = words.astype(jnp.int16)
    short = short_ref.shape
    one, zero = jnp.ones(short, jnp.bfloat16), jnp.zeros(short, jnp.bfloat16)
    for i in range(PLANES):
        table = picked_ref[:, i * width : i * width + LANES].astype(jnp.bfloat16)
        mask = jnp.where(short_ref[...] == jnp.int16(1 << i), one, zero)
        part = jnp.dot(mask, table, preferred_element_type=jnp.float32)
        if i == 0:
            total_ref[...] = part
        else:
            total_ref[...] += part
    return total_ref[...] / jnp.maximum(jnp.concatenate(degrees, axis=0), 1.0)


def mean_first_kernel(width, n_pieces, low_ref, high_ref, local_ref, count_ref, adj_ref, *rest):
    pieces, out_ref = rest[:n_pieces], rest[n_pieces]
    words_ref, short_ref, picked_ref, total_ref, sem, wide_ref = rest[n_pieces + 1 :]
    copies = fetch_words(adj_ref, words_ref, sem)
    pick_blocks(low_ref, high_ref, local_ref, pieces, picked_ref)
    total_ref[...] = mean_rows(count_ref[0], words_ref, copies, short_ref, picked_ref, total_ref, width)
    pack_planes(total_ref, wide_ref, width, BITS)
    out_ref[...] = wide_ref[...].astype(jnp.bfloat16)


def mean_second_kernel(width, n_pieces, low_ref, high_ref, local_ref, count_ref, adj_ref, *rest):
    pieces, (own_ref, out_ref) = rest[:n_pieces], rest[n_pieces : n_pieces + 2]
    words_ref, short_ref, picked_ref, total_ref, sem = rest[n_pieces + 2 :]
    copies = fetch_words(adj_ref, words_ref, sem)
    pick_blocks(low_ref, high_ref, local_ref, pieces, picked_ref)
    mean = mean_rows(count_ref[0], words_ref, copies, short_ref, picked_ref, total_ref, width)
    out_ref[...] = (mean.T[:width, :] + own_ref[...]).astype(jnp.bfloat16)


def here(array):
    return pltpu.with_memory_space_constraint(array, pltpu.VMEM)


def mean_call(kernel, lists, count, adjacency, pieces, more, out_shape, extra, width):
    rows, row_words = adjacency.shape
    lanes = pieces[0].shape[2]
    return pl.pallas_call(
        functools.partial(kernel, width, len(pieces)),
        in_specs=[SMEM] * 4 + [ANY] + [VMEM] * (len(pieces) + len(more)),
        out_specs=VMEM,
        out_shape=out_shape,
        scratch_shapes=[
            pltpu.VMEM((rows, row_words), jnp.int32),
            pltpu.VMEM((rows, row_words), jnp.int16),
            pltpu.VMEM((row_words, lanes), jnp.float32),
            pltpu.VMEM((rows, LANES), jnp.float32),
            pltpu.SemaphoreType.DMA((4,)),
        ]
        + extra,
        compiler_params=PARAMS,
        cost_estimate=pl.CostEstimate(
            flops=2 * rows * row_words * PLANES * LANES, bytes_accessed=4 * rows * row_words, transcendentals=0
        ),
    )(*lists, count, adjacency, *[here(p) for p in pieces], *[here(m) for m in more])


def hidden_kernel(width, classes, self_own, self_far, near_own, near_far, weight_ref, out_weight_ref, hidden_ref, wide_ref, rows_ref, tall_ref, scratch_ref):
    words = self_own.shape[0]
    parts = (self_own, self_far, near_own, near_far)
    for i in range(BITS):
        for n, part in enumerate(parts):
            rows_ref[pl.ds(i * words, words), n * width : (n + 1) * width] = part[:, i * width : (i + 1) * width]
    hidden = jnp.dot(rows_ref[...], weight_ref[...], preferred_element_type=jnp.float32)
    hidden = jnp.maximum(hidden, 0.0).astype(jnp.bfloat16)
    hidden_ref[...] = hidden
    tall_ref[...] = jnp.dot(hidden, out_weight_ref[...], preferred_element_type=jnp.float32)
    scratch_ref[...] = jnp.zeros_like(scratch_ref)
    for i in range(PLANES):
        scratch_ref[:, i * classes : (i + 1) * classes] = tall_ref[pl.ds(i * words, words), :classes]
    wide_ref[...] = scratch_ref[...].astype(jnp.bfloat16)


def own_kernel(seed_ref, weight_ref, *rest):
    hidden_refs, out_ref = rest[:-1], rest[-1]
    total = jnp.zeros(out_ref.shape, jnp.float32)
    for n, hidden_ref in enumerate(hidden_refs):
        rows = hidden_ref.shape[0]
        every = lax.dot_general(
            weight_ref[...], hidden_ref[...], (((1,), (1,)), ((), ())), preferred_element_type=jnp.float32
        )
        high = every.astype(jnp.bfloat16)
        low = (every - high.astype(jnp.float32)).astype(jnp.bfloat16)
        place = lax.broadcasted_iota(jnp.int32, (rows, seed_ref.shape[1]), 0) + n * rows
        chosen = jnp.where(place == seed_ref[...], 1.0, 0.0).astype(jnp.bfloat16)
        total += jnp.dot(high, chosen, preferred_element_type=jnp.float32)
        total += jnp.dot(low, chosen, preferred_element_type=jnp.float32)
    out_ref[...] = total


def per_device(
    grid,
    features,
    self_weight1,
    neigh_weight1,
    need_first,
    count_first,
    adjacency_first,
    self_weight2,
    neigh_weight2,
    need_second,
    count_second,
    adjacency_second,
    seed_rows,
):
    outer, inner, n_col, n_batch = grid
    dom_at, col_at, batch_at = (lax.axis_index(a) for a in MESH_AXES)

    def move(array, which, by):
        return lax.ppermute(array, MESH_AXES, shift_perm(grid, which, by))

    def ring(array, which):
        return [array] + [move(array, which, by) for by in range(1, grid[which])]

    def gather_blocks(piece):
        return [last for first in ring(piece, 0) for second in ring(first, 1) for last in ring(second, 3)]

    def in_order(relative, at):
        n = len(relative)
        ordered = []
        for owner in range(n):
            chosen = relative[0]
            for back in range(1, n):
                chosen = jnp.where((at - owner) % n == back, relative[back], chosen)
            ordered.append(chosen)
        return ordered

    width = features.shape[1]
    rows = adjacency_first.shape[0]
    words = rows // BITS
    lanes = lanes_for(width)
    blocks = rows // BLK

    piece_owner = jnp.stack(
        [
            (((dom_at // inner - ko) % outer) * inner + (dom_at - ki) % inner) * n_batch + (batch_at - kb) % n_batch
            for ko in range(outer)
            for ki in range(inner)
            for kb in range(n_batch)
        ]
    )

    def lists(wanted):
        holder = wanted // blocks
        low = jnp.sum((holder[None, :] < piece_owner[:, None]).astype(jnp.int32), axis=1)
        high = jnp.sum((holder[None, :] <= piece_owner[:, None]).astype(jnp.int32), axis=1)
        return low, high, wanted % blocks

    own = lax.dynamic_slice_in_dim(features, batch_at * rows, rows, 0).reshape(words, BITS * width)
    if lanes > BITS * width:
        own = jnp.pad(own, ((0, 0), (0, lanes - BITS * width)))
    pieces_first = gather_blocks(own.reshape(blocks, WORDS, lanes))

    self_parts = ring(own, 2)
    class_cols = self_weight2.shape[1]
    packed = jnp.concatenate([self_weight1, neigh_weight1, self_weight2.T, neigh_weight2.T], axis=0)
    packs = [in_order(ring(a, 3), batch_at) for a in ring(packed, 2)]
    full = [jnp.concatenate([a[: 2 * width] for a in row], axis=1) for row in packs]
    weight_first = jnp.concatenate([f[:width] for f in full] + [f[width:] for f in full], axis=0)
    rows2 = [[a[2 * width :] for a in row] for row in packs]
    classes = class_cols * n_batch // n_col

    def class_rows(low):
        whole = jnp.concatenate(
            in_order([jnp.concatenate([a[low : low + class_cols] for a in row], axis=0) for row in rows2], col_at),
            axis=1,
        )
        return lax.dynamic_slice_in_dim(whole, col_at * classes, classes, 0)

    weight_own = class_rows(0)
    weight_far = jnp.pad(class_rows(class_cols).T, ((0, 0), (0, LANES - classes)))

    near = mean_call(
        mean_first_kernel,
        lists(need_first[0]),
        count_first,
        adjacency_first,
        pieces_first,
        [],
        pltpu.VMEM((words, lanes), jnp.bfloat16),
        [pltpu.VMEM((words, lanes), jnp.float32)],
        width,
    )
    near_parts = ring(near, 2)
    wide = lanes_for(classes)
    hidden, scores = pl.pallas_call(
        functools.partial(hidden_kernel, width, classes),
        in_specs=[VMEM] * 6,
        out_specs=[VMEM] * 2,
        out_shape=[
            pltpu.VMEM((rows, weight_first.shape[1]), jnp.bfloat16),
            pltpu.VMEM((words, wide), jnp.bfloat16),
        ],
        scratch_shapes=[
            pltpu.VMEM((rows, weight_first.shape[0]), jnp.bfloat16),
            pltpu.VMEM((rows, LANES), jnp.float32),
            pltpu.VMEM((words, wide), jnp.float32),
        ],
        compiler_params=PARAMS,
        name="hidden",
    )(*[here(a) for a in (*self_parts, *near_parts, weight_first, weight_far)])

    pieces_second = gather_blocks(scores.reshape(blocks, WORDS, wide))
    inside = seed_rows % rows
    place = ((batch_at - seed_rows // rows) % n_batch) * rows + (inside % BITS) * words + inside // BITS
    seeds = seed_rows.shape[0]
    own_call = pl.pallas_call(
        own_kernel,
        in_specs=[VMEM] * (2 + n_batch),
        out_specs=VMEM,
        out_shape=pltpu.VMEM((classes, seeds), jnp.float32),
        compiler_params=PARAMS,
        cost_estimate=pl.CostEstimate(
            flops=12 * rows * n_batch * seeds * LANES, bytes_accessed=4 * classes * seeds, transcendentals=0
        ),
        name="own_rows",
    )
    hidden_parts = ring(hidden, 3)
    own_second = own_call(place.reshape(1, seeds), weight_own, *[here(h) for h in hidden_parts])
    half = mean_call(
        mean_second_kernel,
        lists(need_second[0]),
        count_second,
        adjacency_second,
        pieces_second,
        [own_second],
        pltpu.VMEM((classes, seeds), jnp.bfloat16),
        [],
        classes,
    )
    logits = jnp.concatenate(in_order(ring(half, 2), col_at), axis=0)
    return logits.astype(jnp.float32).T


def solution(mesh):
    sizes = tuple(mesh.shape[a] for a in MESH_AXES)
    inner = 2 if sizes[0] % 2 == 0 else 1
    grid = (sizes[0] // inner, inner, sizes[1], sizes[2])
    placed = (
        P("dom", "col"),
        P("col", "batch"),
        P("col", "batch"),
        P(("dom", "batch"), None),
        P(("dom", "batch")),
        P(("dom", "batch"), None),
        P("col", "batch"),
        P("col", "batch"),
        P(("dom", "batch"), None),
        P(("dom", "batch")),
        P(("dom", "batch"), None),
        P(("dom", "batch")),
    )

    def body(*args):
        return per_device(grid, *args)

    return jax.shard_map(
        body, mesh=mesh, in_specs=placed, out_specs=P(("dom", "batch"), None), check_vma=False
    )
```

```python
import functools

import jax
import jax.numpy as jnp
from jax import lax
from jax.experimental import pallas as pl
from jax.experimental.pallas import tpu as pltpu
from jax.sharding import PartitionSpec as P


BLK = 128
BITS = 16
PLANES = 15
WORDS = BLK // BITS
LANES = 128
MESH_AXES = ("dom", "col", "batch")
VMEM = pl.BlockSpec(memory_space=pltpu.VMEM)
SMEM = pl.BlockSpec(memory_space=pltpu.SMEM)
ANY = pl.BlockSpec(memory_space=pl.ANY)
PARAMS = pltpu.CompilerParams(vmem_limit_bytes=20 * 2**20)


def lanes_for(width):
    need = max((PLANES - 1) * width + LANES, BITS * width if width % 64 == 0 else 0)
    return -(-need // LANES) * LANES


def paired(size):
    return size & (size - 1) == 0


def shift_perm(sizes, which, by):
    pairs = []
    total = 1
    for size in sizes:
        total *= size
    for source in range(total):
        place = []
        rest = source
        for size in reversed(sizes):
            place.append(rest % size)
            rest //= size
        place = place[::-1]
        size = sizes[which]
        place[which] = place[which] ^ by if paired(size) else (place[which] + by) % size
        target = 0
        for size, at in zip(sizes, place):
            target = target * size + at
        pairs.append((source, target))
    return pairs


def pack_planes(tall_ref, out_ref, width, planes):
    words = out_ref.shape[0]
    for i in range(planes):
        piece = tall_ref[pl.ds(i, words, stride=BITS), :]
        out_ref[:, i * width : (i + 1) * width] = piece[:, :width]


def fetch_words(adj_ref, words_ref, sem):
    rows = adj_ref.shape[0] // sem.shape[0]
    copies = [
        pltpu.make_async_copy(adj_ref.at[pl.ds(n * rows, rows)], words_ref.at[pl.ds(n * rows, rows)], sem.at[n])
        for n in range(sem.shape[0])
    ]
    for copy in copies:
        copy.start()
    return copies


def behind(at, by, size):
    return lax.bitwise_xor(at, jnp.int32(by)) if paired(size) else lax.rem(at + size - by, size)


def owner_of(grid, piece, place_ref):
    outer, inner, _, n_batch = grid
    ko, ki, kb = piece // (inner * n_batch), piece // n_batch % inner, piece % n_batch
    dom_at, batch_at = place_ref[0], place_ref[2]
    outer_at = behind(lax.div(dom_at, inner), ko, outer)
    inner_at = behind(lax.rem(dom_at, inner), ki, inner)
    return (outer_at * inner + inner_at) * n_batch + behind(batch_at, kb, n_batch)


def invert(need_ref, inverse_ref):
    listed = need_ref.shape[0]

    def clear(g, _):
        inverse_ref[g] = listed
        return 0

    def enter(b, _):
        inverse_ref[need_ref[b]] = b
        return 0

    lax.fori_loop(0, inverse_ref.shape[0], clear, 0, unroll=8)
    lax.fori_loop(0, listed, enter, 0, unroll=8)


def pick_blocks(grid, place_ref, inverse_ref, pieces, picked_ref, cleared=()):
    for n, piece in pieces:
        blocks = piece.shape[0]
        owner = owner_of(grid, n, place_ref)
        for k in range(blocks):
            at = pl.multiple_of(inverse_ref[owner * blocks + k] * WORDS, WORDS)
            picked_ref[pl.ds(at, WORDS), :] = piece[k].astype(jnp.float32)
    for n in cleared:
        owner = owner_of(grid, n, place_ref)
        for k in range(blocks):
            at = pl.multiple_of(inverse_ref[owner * blocks + k] * WORDS, WORDS)
            picked_ref[pl.ds(at, WORDS), :] = jnp.zeros((WORDS, picked_ref.shape[1]), jnp.float32)


def below(need_ref, bound):
    def add(b, total):
        return total + jnp.where(need_ref[b] < bound, 1, 0)

    return lax.fori_loop(0, need_ref.shape[0], add, 0, unroll=8)


def turns_of(outer):
    return list(range(1, outer))


def late_parts(grid):
    outer, inner, _, n_batch = grid
    return [
        [(ko * inner + inner - 1) * n_batch + kb for kb in range(n_batch)] for ko in ([0] + turns_of(outer))[-1:]
    ]


def late_spans(grid, blocks, place_ref, need_ref):
    n_batch = grid[3]
    spans = []
    for part in late_parts(grid):
        first = lax.div(owner_of(grid, part[0], place_ref), n_batch) * (n_batch * blocks)
        spans.append((below(need_ref, first), below(need_ref, first + n_batch * blocks)))
    return spans


def multiply_planes(short_ref, picked_ref, total_ref, width):
    short = short_ref.shape
    one, zero = jnp.ones(short, jnp.bfloat16), jnp.zeros(short, jnp.bfloat16)
    joined = max(1, 256 // short[1])
    for i in range(0, PLANES, joined):
        masks, tables = [], []
        for k in range(i, min(i + joined, PLANES)):
            tables.append(picked_ref[: short[1], k * width : k * width + LANES].astype(jnp.bfloat16))
            masks.append(jnp.where(short_ref[...] == jnp.int16(1 << k), one, zero))
        mask, table = jnp.concatenate(masks, axis=1), jnp.concatenate(tables, axis=0)
        part = jnp.dot(mask, table, preferred_element_type=jnp.float32)
        if i == 0:
            total_ref[...] = part
        else:
            total_ref[...] += part


def mean_kernel(grid, width, n_pieces, place_ref, need_ref, count_ref, adj_ref, *rest):
    pieces, out_ref = rest[:n_pieces], rest[n_pieces]
    words_ref, short_ref, picked_ref, total_ref, wide_ref, inverse_ref, sem = rest[n_pieces + 1 :]
    copies = fetch_words(adj_ref, words_ref, sem)
    invert(need_ref, inverse_ref)
    pick_blocks(grid, place_ref, inverse_ref, list(enumerate(pieces)), picked_ref)
    rows = words_ref.shape[0] // len(copies)
    degrees = []
    for n, copy in enumerate(copies):
        copy.wait()
        words = words_ref[n * rows : (n + 1) * rows, :]
        column = lax.broadcasted_iota(jnp.int32, words.shape, 1)
        words = jnp.where(column < count_ref[0] * WORDS, words, 0)
        degrees.append(jnp.sum(jnp.where(words != 0, 1.0, 0.0), axis=1, keepdims=True))
        short_ref[n * rows : (n + 1) * rows, :] = words.astype(jnp.int16)
    multiply_planes(short_ref, picked_ref, total_ref, width)
    total_ref[...] = total_ref[...] / jnp.maximum(jnp.concatenate(degrees, axis=0), 1.0)
    pack_planes(total_ref, wide_ref, width, BITS)
    out_ref[...] = wide_ref[...].astype(jnp.bfloat16)


def prepare_kernel(grid, blocks, place_ref, need_ref, count_ref, adj_ref, short_ref, late_ref, degree_ref, words_ref, sem):
    copies = fetch_words(adj_ref, words_ref, sem)
    spans = late_spans(grid, blocks, place_ref, need_ref)
    rows = words_ref.shape[0] // len(copies)
    whole = words_ref.shape[1]
    window = late_ref.shape[1] // len(spans)
    for n, copy in enumerate(copies):
        copy.wait()
        at = slice(n * rows, (n + 1) * rows)
        words = words_ref[at, :]
        column = lax.broadcasted_iota(jnp.int32, words.shape, 1)
        words = jnp.where(column < count_ref[0] * WORDS, words, 0)
        degree = jnp.sum(jnp.where(words != 0, 1.0, 0.0), axis=1, keepdims=True)
        degree_ref[at, :] = jnp.broadcast_to(jnp.maximum(degree, 1.0), (rows, LANES))
        early = words
        for k, (low, high) in enumerate(spans):
            early = jnp.where((column >= low * WORDS) & (column < high * WORDS), 0, early)
            turned = pltpu.roll(words, lax.rem(whole - low * WORDS, whole), 1)[:, :window]
            inside = lax.broadcasted_iota(jnp.int32, turned.shape, 1) < (high - low) * WORDS
            late_ref[at, k * window : (k + 1) * window] = jnp.where(inside, turned, 0)
        short_ref[at, :] = early.astype(jnp.int16)


def main_kernel(grid, width, n_pieces, place_ref, need_ref, short_ref, *rest):
    late = [n for part in late_parts(grid) for n in part]
    early = [n for n in range(n_pieces) if n not in late]
    pieces, total_ref = rest[: len(early)], rest[len(early)]
    picked_ref, inverse_ref = rest[len(early) + 1 :]
    invert(need_ref, inverse_ref)
    pick_blocks(grid, place_ref, inverse_ref, list(zip(early, pieces)), picked_ref, late)
    multiply_planes(short_ref, picked_ref, total_ref, width)


def late_kernel(grid, width, place_ref, need_ref, words_ref, degree_ref, main_ref, own_ref, *rest):
    parts = late_parts(grid)
    n_late = sum(len(part) for part in parts)
    pieces, out_ref = rest[:n_late], rest[n_late]
    picked_ref, short_ref, total_ref, inverse_ref = rest[n_late + 1 :]
    blocks = pieces[0].shape[0]
    picked_ref[...] = jnp.zeros_like(picked_ref)
    invert(need_ref, inverse_ref)
    spans = late_spans(grid, blocks, place_ref, need_ref)
    listed = need_ref.shape[0]
    window = words_ref.shape[1] // len(parts) // WORDS
    spare = len(parts) * window
    used = 0
    for k, part in enumerate(parts):
        for n in part:
            owner = owner_of(grid, n, place_ref)
            for g in range(blocks):
                at = inverse_ref[owner * blocks + g]
                at = jnp.where(at == listed, spare, at - spans[k][0] + k * window)
                picked_ref[pl.ds(pl.multiple_of(at * WORDS, WORDS), WORDS), :] = pieces[used][g].astype(jnp.float32)
            used += 1
    short_ref[...] = words_ref[...].astype(jnp.int16)
    multiply_planes(short_ref, picked_ref, total_ref, width)
    mean = (main_ref[...] + total_ref[...]) / degree_ref[...]
    out_ref[...] = (mean.T + own_ref[...])[:width, :].astype(jnp.bfloat16)


def here(array):
    return pltpu.with_memory_space_constraint(array, pltpu.VMEM)


def cost(flops, count):
    return pl.CostEstimate(flops=flops, bytes_accessed=count, transcendentals=0)


def stay(array):
    return pltpu.with_memory_space_constraint(array, pltpu.HBM)


def mean_call(grid, place, need, count, adjacency, pieces, width):
    rows, row_words = adjacency.shape
    blocks, _, lanes = pieces[0].shape
    return pl.pallas_call(
        functools.partial(mean_kernel, grid, width, len(pieces)),
        in_specs=[SMEM] * 3 + [ANY] + [VMEM] * len(pieces),
        out_specs=VMEM,
        out_shape=pltpu.VMEM((rows // BITS, lanes), jnp.bfloat16),
        scratch_shapes=[
            pltpu.VMEM((rows, row_words), jnp.int32),
            pltpu.VMEM((rows, row_words), jnp.int16),
            pltpu.VMEM((row_words + WORDS, lanes), jnp.float32),
            pltpu.VMEM((rows, LANES), jnp.float32),
            pltpu.VMEM((rows // BITS, lanes), jnp.float32),
            pltpu.SMEM((len(pieces) * blocks,), jnp.int32),
            pltpu.SemaphoreType.DMA((4,)),
        ],
        compiler_params=PARAMS,
        cost_estimate=cost(2 * rows * row_words * PLANES * LANES, 4 * rows * row_words),
        name="mean_first",
    )(place, need, count, stay(adjacency), *[here(p) for p in pieces])


def prepare_call(grid, place, need, count, adjacency, blocks):
    rows, row_words = adjacency.shape
    window = min(grid[3] * blocks * WORDS, row_words) * len(late_parts(grid))
    return pl.pallas_call(
        functools.partial(prepare_kernel, grid, blocks),
        in_specs=[SMEM] * 3 + [ANY],
        out_specs=[VMEM] * 3,
        out_shape=[
            pltpu.VMEM((rows, row_words), jnp.int16),
            pltpu.VMEM((rows, window), jnp.int32),
            pltpu.VMEM((rows, LANES), jnp.float32),
        ],
        scratch_shapes=[pltpu.VMEM((rows, row_words), jnp.int32), pltpu.SemaphoreType.DMA((4,))],
        compiler_params=PARAMS,
        cost_estimate=cost(2 * rows * row_words * LANES, 4 * rows * row_words),
        name="prepare",
    )(place, need, count, stay(adjacency))


def split_mean_calls(grid, place, need, prepared, pieces, own, width):
    short, late_words, degree = prepared
    rows, row_words = short.shape
    blocks, _, lanes = pieces[0].shape
    late = [n for part in late_parts(grid) for n in part]
    early = [n for n in range(len(pieces)) if n not in late]
    inverse = pltpu.SMEM((len(pieces) * blocks,), jnp.int32)
    total = pl.pallas_call(
        functools.partial(main_kernel, grid, width, len(pieces)),
        in_specs=[SMEM] * 2 + [VMEM] * (1 + len(early)),
        out_specs=VMEM,
        out_shape=pltpu.VMEM((rows, LANES), jnp.float32),
        scratch_shapes=[pltpu.VMEM((row_words + WORDS, lanes), jnp.float32), inverse],
        compiler_params=PARAMS,
        cost_estimate=cost(2 * rows * row_words * PLANES * LANES, 4 * rows * row_words),
        name="mean_main",
    )(place, need, here(short), *[here(pieces[n]) for n in early])
    late_cols = late_words.shape[1]
    return pl.pallas_call(
        functools.partial(late_kernel, grid, width),
        in_specs=[SMEM] * 2 + [VMEM] * (4 + len(late)),
        out_specs=VMEM,
        out_shape=pltpu.VMEM((width, rows), jnp.bfloat16),
        scratch_shapes=[
            pltpu.VMEM((late_cols + WORDS, lanes), jnp.float32),
            pltpu.VMEM((rows, late_cols), jnp.int16),
            pltpu.VMEM((rows, LANES), jnp.float32),
            inverse,
        ],
        compiler_params=PARAMS,
        cost_estimate=cost(2 * rows * late_cols * PLANES * LANES, 4 * rows * LANES),
        name="mean_late",
    )(place, need, here(late_words), here(degree), here(total), here(own), *[here(pieces[n]) for n in late])


def picked_by(values, at):
    chosen = values[0]
    for n in range(1, len(values)):
        chosen = jnp.where(at == n, values[n], chosen)
    return chosen


def hidden_kernel(width, classes, spare, grid, place_ref, *rest):
    _, _, n_col, n_batch = grid
    n_parts = 2 * n_col
    parts, packs = rest[:n_parts], rest[n_parts : n_parts + n_col * n_batch]
    hidden_ref, wide_ref, own_weight_ref, rows_ref, tall_ref, scratch_ref = rest[n_parts + n_col * n_batch :]
    col_at, batch_at = place_ref[1], place_ref[2]
    words = parts[0].shape[0]

    def weights(back, owner, low, count):
        found = [packs[back * n_batch + k][low : low + count, :] for k in range(n_batch)]
        return picked_by(found, lax.rem(batch_at + n_batch - owner, n_batch))

    first = [
        jnp.concatenate([weights(back, owner, half * width, width) for owner in range(n_batch)], axis=1)
        for half in range(2)
        for back in range(n_col)
    ]

    def class_weights(low):
        by_back = [weights(back, col_at, low, spare) for back in range(n_col)]
        return jnp.concatenate(
            [picked_by(by_back, lax.rem(col_at + n_col - owner, n_col)) for owner in range(n_col)], axis=1
        )

    own_weight_ref[...] = class_weights(2 * width)
    far_weight = class_weights(2 * width + spare)
    for i in range(BITS):
        for n, part in enumerate(parts):
            rows_ref[pl.ds(i * words, words), n * width : (n + 1) * width] = part[:, i * width : (i + 1) * width]
    hidden = jnp.dot(rows_ref[...], jnp.concatenate(first, axis=0), preferred_element_type=jnp.float32)
    hidden = jnp.maximum(hidden, 0.0).astype(jnp.bfloat16)
    hidden_ref[...] = hidden
    tall_ref[...] = lax.dot_general(
        hidden, far_weight, (((1,), (1,)), ((), ())), preferred_element_type=jnp.float32
    )
    scratch_ref[...] = jnp.zeros_like(scratch_ref)
    for i in range(PLANES):
        scratch_ref[:, i * classes : (i + 1) * classes] = tall_ref[pl.ds(i * words, words), :classes]
    wide_ref[...] = scratch_ref[...].astype(jnp.bfloat16)


def own_kernel(seed_ref, weight_ref, *rest):
    hidden_refs, out_ref = rest[:-1], rest[-1]
    total = jnp.zeros((weight_ref.shape[0], out_ref.shape[1]), jnp.float32)
    for n, hidden_ref in enumerate(hidden_refs):
        rows = hidden_ref.shape[0]
        every = lax.dot_general(
            weight_ref[...], hidden_ref[...], (((1,), (1,)), ((), ())), preferred_element_type=jnp.float32
        )
        high = every.astype(jnp.bfloat16)
        low = (every - high.astype(jnp.float32)).astype(jnp.bfloat16)
        place = lax.broadcasted_iota(jnp.int32, (rows, seed_ref.shape[1]), 0) + n * rows
        chosen = jnp.where(place == seed_ref[...], 1.0, 0.0).astype(jnp.bfloat16)
        total += jnp.dot(high, chosen, preferred_element_type=jnp.float32)
        total += jnp.dot(low, chosen, preferred_element_type=jnp.float32)
    out_ref[...] = jnp.zeros_like(out_ref)
    out_ref[: total.shape[0], :] = total


def per_device(
    grid,
    features,
    self_weight1,
    neigh_weight1,
    need_first,
    count_first,
    adjacency_first,
    self_weight2,
    neigh_weight2,
    need_second,
    count_second,
    adjacency_second,
    seed_rows,
):
    _, _, n_col, n_batch = grid
    dom_at, col_at, batch_at = (lax.axis_index(a) for a in MESH_AXES)

    def move(array, which, by):
        return lax.ppermute(array, MESH_AXES, shift_perm(grid, which, by))

    def ring(array, which):
        return [array] + [move(array, which, by) for by in range(1, grid[which])]

    def gather_blocks(piece):
        return [last for first in ring(piece, 0) for second in ring(first, 1) for last in ring(second, 3)]

    def in_order(relative, at):
        n = len(relative)
        ordered = []
        for owner in range(n):
            chosen = relative[0]
            for back in range(1, n):
                chosen = jnp.where((at - owner) % n == back, relative[back], chosen)
            ordered.append(chosen)
        return ordered

    width = features.shape[1]
    rows = adjacency_first.shape[0]
    words = rows // BITS
    lanes = lanes_for(width)
    blocks = rows // BLK

    place = jnp.stack([dom_at, col_at, batch_at])
    prepared = prepare_call(grid, place, need_second[0], count_second, adjacency_second, blocks)

    own = lax.dynamic_slice_in_dim(features, batch_at * rows, rows, 0).reshape(words, BITS * width)
    if lanes > BITS * width:
        own = jnp.pad(own, ((0, 0), (0, lanes - BITS * width)))
    pieces_first = gather_blocks(own.reshape(blocks, WORDS, lanes))

    self_parts = ring(own, 2)
    class_cols = self_weight2.shape[1]
    classes = class_cols * n_batch // n_col
    spare = -(-class_cols // 16) * 16
    tall2 = [jnp.pad(w.T, ((0, spare - class_cols), (0, 0))) for w in (self_weight2, neigh_weight2)]
    packed = jnp.concatenate([self_weight1, neigh_weight1, *tall2], axis=0)
    packs = [p for a in ring(packed, 2) for p in ring(a, 3)]

    near = mean_call(grid, place, need_first[0], count_first, adjacency_first, pieces_first, width)
    near_parts = ring(near, 2)
    wide = lanes_for(classes)
    hidden_cols = self_weight1.shape[1] * n_batch
    hidden, scores, weight_own = pl.pallas_call(
        functools.partial(hidden_kernel, width, classes, spare, grid),
        in_specs=[SMEM] + [VMEM] * (2 * n_col + n_col * n_batch),
        out_specs=[VMEM] * 3,
        out_shape=[
            pltpu.VMEM((rows, hidden_cols), jnp.bfloat16),
            pltpu.VMEM((words, wide), jnp.bfloat16),
            pltpu.VMEM((spare, hidden_cols), jnp.bfloat16),
        ],
        scratch_shapes=[
            pltpu.VMEM((rows, 2 * n_col * width), jnp.bfloat16),
            pltpu.VMEM((rows, spare), jnp.float32),
            pltpu.VMEM((words, wide), jnp.float32),
        ],
        compiler_params=PARAMS,
        name="hidden",
    )(place, *[here(a) for a in (*self_parts, *near_parts, *packs)])

    pieces_second = gather_blocks(scores.reshape(blocks, WORDS, wide))
    inside = seed_rows % rows
    seed_at = ((batch_at - seed_rows // rows) % n_batch) * rows + (inside % BITS) * words + inside // BITS
    seeds = seed_rows.shape[0]
    own_call = pl.pallas_call(
        own_kernel,
        in_specs=[VMEM] * (2 + n_batch),
        out_specs=VMEM,
        out_shape=pltpu.VMEM((LANES, seeds), jnp.float32),
        compiler_params=PARAMS,
        cost_estimate=pl.CostEstimate(
            flops=12 * rows * n_batch * seeds * LANES, bytes_accessed=4 * classes * seeds, transcendentals=0
        ),
        name="own_rows",
    )
    hidden_parts = ring(hidden, 3)
    own_second = own_call(seed_at.reshape(1, seeds), here(weight_own), *[here(h) for h in hidden_parts])
    half = split_mean_calls(grid, place, need_second[0], prepared, pieces_second, own_second, classes)
    logits = jnp.concatenate(in_order(ring(half, 2), col_at), axis=0)
    return logits.astype(jnp.float32).T


def solution(mesh):
    sizes = tuple(mesh.shape[a] for a in MESH_AXES)
    inner = 2 if sizes[0] % 2 == 0 else 1
    grid = (sizes[0] // inner, inner, sizes[1], sizes[2])
    placed = (
        P("dom", "col"),
        P("col", "batch"),
        P("col", "batch"),
        P(("dom", "batch"), None),
        P(("dom", "batch")),
        P(("dom", "batch"), None),
        P("col", "batch"),
        P("col", "batch"),
        P(("dom", "batch"), None),
        P(("dom", "batch")),
        P(("dom", "batch"), None),
        P(("dom", "batch")),
    )

    def body(*args):
        return per_device(grid, *args)

    return jax.shard_map(
        body, mesh=mesh, in_specs=placed, out_specs=P(("dom", "batch"), None), check_vma=False
    )
```

```python
import functools

import jax
import jax.numpy as jnp
from jax import lax
from jax.experimental import pallas as pl
from jax.experimental.pallas import tpu as pltpu
from jax.sharding import PartitionSpec as P


BLK = 128
BITS = 16
PLANES = 15
WORDS = BLK // BITS
LANES = 128
MESH_AXES = ("dom", "col", "batch")
VMEM = pl.BlockSpec(memory_space=pltpu.VMEM)
SMEM = pl.BlockSpec(memory_space=pltpu.SMEM)
ANY = pl.BlockSpec(memory_space=pl.ANY)
PARAMS = pltpu.CompilerParams(vmem_limit_bytes=20 * 2**20)


def lanes_for(width):
    return -(-max((PLANES - 1) * width + LANES, PLANES * width) // LANES) * LANES


def tiles_for(width, blocks):
    full, left = divmod(PLANES * width, LANES)
    if left * blocks > LANES or left == 0 or LANES % blocks:
        return -(-PLANES * width // LANES), 0
    return full, left


def paired(size):
    return size & (size - 1) == 0


def shift_perm(sizes, which, by):
    pairs = []
    total = 1
    for size in sizes:
        total *= size
    for source in range(total):
        place = []
        rest = source
        for size in reversed(sizes):
            place.append(rest % size)
            rest //= size
        place = place[::-1]
        size = sizes[which]
        place[which] = place[which] ^ by if paired(size) else (place[which] + by) % size
        target = 0
        for size, at in zip(sizes, place):
            target = target * size + at
        pairs.append((source, target))
    return pairs


def pack_planes(tall_ref, out_ref, width, planes):
    words = out_ref.shape[0]
    for i in range(planes):
        piece = tall_ref[pl.ds(i, words, stride=BITS), :]
        out_ref[:, i * width : (i + 1) * width] = piece[:, :width]


def fetch_words(adj_ref, words_ref, sem):
    rows = adj_ref.shape[0] // sem.shape[0]
    copies = [
        pltpu.make_async_copy(adj_ref.at[pl.ds(n * rows, rows)], words_ref.at[pl.ds(n * rows, rows)], sem.at[n])
        for n in range(sem.shape[0])
    ]
    for copy in copies:
        copy.start()
    return copies


def behind(at, by, size):
    return at ^ by if paired(size) else lax.rem(at + size - by, size)


def owner_of(grid, piece, place_ref):
    outer, inner, _, n_batch = grid
    ko, ki, kb = piece // (inner * n_batch), piece // n_batch % inner, piece % n_batch
    dom_at, batch_at = place_ref[0], place_ref[2]
    outer_at = behind(lax.div(dom_at, inner), ko, outer)
    inner_at = behind(lax.rem(dom_at, inner), ki, inner)
    return (outer_at * inner + inner_at) * n_batch + behind(batch_at, kb, n_batch)


def invert(need_ref, inverse_ref):
    listed = need_ref.shape[0]

    def clear(g, _):
        inverse_ref[g] = listed
        return 0

    def enter(b, _):
        inverse_ref[need_ref[b]] = b
        return 0

    lax.fori_loop(0, inverse_ref.shape[0], clear, 0, unroll=8)
    lax.fori_loop(0, listed, enter, 0, unroll=8)


def put_block(piece, k, blocks, width, picked_ref, at):
    tiles, left = tiles_for(width, blocks)
    for t in range(tiles):
        picked_ref[pl.ds(at, WORDS), t * LANES : (t + 1) * LANES] = piece[k * tiles + t].astype(jnp.float32)
    if left:
        shared = piece[blocks * tiles].astype(jnp.float32)
        turned = pltpu.roll(shared, (LANES - k * (LANES // blocks)) % LANES, 1) if k else shared
        picked_ref[pl.ds(at, WORDS), tiles * LANES : (tiles + 1) * LANES] = turned


def pick_blocks(blocks, width, spot, pieces, picked_ref, cleared=()):
    for n, piece in pieces:
        for k in range(blocks):
            put_block(piece, k, blocks, width, picked_ref, pl.multiple_of(spot(n, k) * WORDS, WORDS))
    for n in cleared:
        for k in range(blocks):
            at = pl.multiple_of(spot(n, k) * WORDS, WORDS)
            picked_ref[pl.ds(at, WORDS), :] = jnp.zeros((WORDS, picked_ref.shape[1]), jnp.float32)


def below(need_ref, bound):
    def add(b, total):
        return total + jnp.where(need_ref[b] < bound, 1, 0)

    return lax.fori_loop(0, need_ref.shape[0], add, 0, unroll=8)


def turns_of(outer):
    return list(range(1, outer))


def late_parts(grid):
    outer, inner, _, n_batch = grid
    return [
        [(ko * inner + inner - 1) * n_batch + kb for kb in range(n_batch)] for ko in ([0] + turns_of(outer))[-1:]
    ]


def late_spans(grid, blocks, place_ref, need_ref):
    n_batch = grid[3]
    spans = []
    for part in late_parts(grid):
        first = lax.div(owner_of(grid, part[0], place_ref), n_batch) * (n_batch * blocks)
        spans.append((below(need_ref, first), below(need_ref, first + n_batch * blocks)))
    return spans


def multiply_planes(short_ref, picked_ref, total_ref, width):
    short = short_ref.shape
    one, zero = jnp.ones(short, jnp.bfloat16), jnp.zeros(short, jnp.bfloat16)
    joined = max(1, 256 // short[1])
    for i in range(0, PLANES, joined):
        masks, tables = [], []
        for k in range(i, min(i + joined, PLANES)):
            tables.append(picked_ref[: short[1], k * width : k * width + LANES].astype(jnp.bfloat16))
            masks.append(jnp.where(short_ref[...] == jnp.int16(1 << k), one, zero))
        mask, table = jnp.concatenate(masks, axis=1), jnp.concatenate(tables, axis=0)
        part = jnp.dot(mask, table, preferred_element_type=jnp.float32)
        if i == 0:
            total_ref[...] = part
        else:
            total_ref[...] += part


def mean_kernel(grid, width, n_pieces, place_ref, need_ref, count_ref, adj_ref, *rest):
    pieces, out_ref = rest[:n_pieces], rest[n_pieces]
    words_ref, short_ref, picked_ref, total_ref, wide_ref, inverse_ref, sem = rest[n_pieces + 1 :]
    copies = fetch_words(adj_ref, words_ref, sem)
    invert(need_ref, inverse_ref)
    blocks = inverse_ref.shape[0] // n_pieces
    owners = [owner_of(grid, n, place_ref) for n in range(n_pieces)]
    pick_blocks(blocks, width, lambda n, k: inverse_ref[owners[n] * blocks + k], list(enumerate(pieces)), picked_ref)
    rows = words_ref.shape[0] // len(copies)
    degrees = []
    for n, copy in enumerate(copies):
        copy.wait()
        words = words_ref[n * rows : (n + 1) * rows, :]
        column = lax.broadcasted_iota(jnp.int32, words.shape, 1)
        words = jnp.where(column < count_ref[0] * WORDS, words, 0)
        degrees.append(jnp.sum(jnp.where(words != 0, 1.0, 0.0), axis=1, keepdims=True))
        short_ref[n * rows : (n + 1) * rows, :] = words.astype(jnp.int16)
    multiply_planes(short_ref, picked_ref, total_ref, width)
    total_ref[...] = total_ref[...] / jnp.maximum(jnp.concatenate(degrees, axis=0), 1.0)
    pack_planes(total_ref, wide_ref, width, BITS)
    out_ref[...] = wide_ref[...].astype(jnp.bfloat16)


def prepare_kernel(
    grid, blocks, place_ref, need_ref, count_ref, adj_ref, short_ref, late_ref, degree_ref, spot_ref, words_ref, inverse_ref, sem
):
    copies = fetch_words(adj_ref, words_ref, sem)
    spans = late_spans(grid, blocks, place_ref, need_ref)
    invert(need_ref, inverse_ref)
    listed = need_ref.shape[0]
    parts = late_parts(grid)
    total = inverse_ref.shape[0]
    for n in range(total // blocks):
        owner = owner_of(grid, n, place_ref)
        for k in range(blocks):
            spot_ref[n * blocks + k] = inverse_ref[owner * blocks + k]
    wide = late_ref.shape[1] // len(parts) // WORDS
    used = total
    for j, part in enumerate(parts):
        for n in part:
            for k in range(blocks):
                at = spot_ref[n * blocks + k]
                spot_ref[used] = jnp.where(at == listed, len(parts) * wide, at - spans[j][0] + j * wide)
                used += 1
    rows = words_ref.shape[0] // len(copies)
    whole = words_ref.shape[1]
    window = late_ref.shape[1] // len(spans)
    for n, copy in enumerate(copies):
        copy.wait()
        at = slice(n * rows, (n + 1) * rows)
        words = words_ref[at, :]
        column = lax.broadcasted_iota(jnp.int32, words.shape, 1)
        words = jnp.where(column < count_ref[0] * WORDS, words, 0)
        degree = jnp.sum(jnp.where(words != 0, 1.0, 0.0), axis=1, keepdims=True)
        degree_ref[at, :] = jnp.broadcast_to(jnp.maximum(degree, 1.0), (rows, LANES))
        early = words
        for k, (low, high) in enumerate(spans):
            early = jnp.where((column >= low * WORDS) & (column < high * WORDS), 0, early)
            turned = pltpu.roll(words, lax.rem(whole - low * WORDS, whole), 1)[:, :window]
            inside = lax.broadcasted_iota(jnp.int32, turned.shape, 1) < (high - low) * WORDS
            late_ref[at, k * window : (k + 1) * window] = jnp.where(inside, turned, 0)
        short_ref[at, :] = early.astype(jnp.int16)


def main_kernel(grid, width, blocks, n_pieces, spot_ref, short_ref, *rest):
    late = [n for part in late_parts(grid) for n in part]
    early = [n for n in range(n_pieces) if n not in late]
    pieces, total_ref, picked_ref = rest[: len(early)], rest[len(early)], rest[len(early) + 1]
    pick_blocks(blocks, width, lambda n, k: spot_ref[n * blocks + k], list(zip(early, pieces)), picked_ref, late)
    multiply_planes(short_ref, picked_ref, total_ref, width)


def late_kernel(width, blocks, first_row, spot_ref, words_ref, degree_ref, main_ref, own_ref, *rest):
    pieces, out_ref = rest[:-4], rest[-4]
    picked_ref, short_ref, total_ref = rest[-3:]
    rows = pl.ds(first_row, out_ref.shape[1])
    picked_ref[...] = jnp.zeros_like(picked_ref)
    base = spot_ref.shape[0] - len(pieces) * blocks
    pick_blocks(blocks, width, lambda n, k: spot_ref[base + n * blocks + k], list(enumerate(pieces)), picked_ref)
    short_ref[...] = words_ref[rows, :].astype(jnp.int16)
    multiply_planes(short_ref, picked_ref, total_ref, width)
    mean = (main_ref[rows, :] + total_ref[...]) / degree_ref[rows, :]
    out_ref[...] = (mean.T + own_ref[:, rows])[:width, :].astype(jnp.bfloat16)


def here(array):
    return pltpu.with_memory_space_constraint(array, pltpu.VMEM)


def cost(flops, count):
    return pl.CostEstimate(flops=flops, bytes_accessed=count, transcendentals=0)


def stay(array):
    return pltpu.with_memory_space_constraint(array, pltpu.HBM)


def mean_call(grid, place, need, count, adjacency, pieces, blocks, width):
    rows, row_words = adjacency.shape
    lanes = lanes_for(width)
    return pl.pallas_call(
        functools.partial(mean_kernel, grid, width, len(pieces)),
        in_specs=[SMEM] * 3 + [ANY] + [VMEM] * len(pieces),
        out_specs=VMEM,
        out_shape=pltpu.VMEM((rows // BITS, BITS * width), jnp.bfloat16),
        scratch_shapes=[
            pltpu.VMEM((rows, row_words), jnp.int32),
            pltpu.VMEM((rows, row_words), jnp.int16),
            pltpu.VMEM((row_words + WORDS, lanes), jnp.float32),
            pltpu.VMEM((rows, LANES), jnp.float32),
            pltpu.VMEM((rows // BITS, BITS * width), jnp.float32),
            pltpu.SMEM((len(pieces) * blocks,), jnp.int32),
            pltpu.SemaphoreType.DMA((4,)),
        ],
        compiler_params=PARAMS,
        cost_estimate=cost(2 * rows * row_words * PLANES * LANES, 4 * rows * row_words),
        name="mean_first",
    )(place, need, count, stay(adjacency), *[here(p) for p in pieces])


def prepare_call(grid, place, need, count, adjacency, blocks):
    rows, row_words = adjacency.shape
    parts = late_parts(grid)
    window = min(grid[3] * blocks * WORDS, row_words) * len(parts)
    total = grid[0] * grid[1] * grid[3] * blocks
    return pl.pallas_call(
        functools.partial(prepare_kernel, grid, blocks),
        in_specs=[SMEM] * 3 + [ANY],
        out_specs=[VMEM] * 3 + [SMEM],
        out_shape=[
            pltpu.VMEM((rows, row_words), jnp.int16),
            pltpu.VMEM((rows, window), jnp.int32),
            pltpu.VMEM((rows, LANES), jnp.float32),
            jax.ShapeDtypeStruct((total + len(parts) * grid[3] * blocks,), jnp.int32),
        ],
        scratch_shapes=[
            pltpu.VMEM((rows, row_words), jnp.int32),
            pltpu.SMEM((total,), jnp.int32),
            pltpu.SemaphoreType.DMA((4,)),
        ],
        compiler_params=PARAMS,
        cost_estimate=cost(2 * rows * row_words * LANES, 4 * rows * row_words),
        name="prepare",
    )(place, need, count, stay(adjacency))


def split_mean_calls(grid, prepared, pieces, own, blocks, width):
    short, late_words, degree, spot = prepared
    rows, row_words = short.shape
    lanes = lanes_for(width)
    late = [n for part in late_parts(grid) for n in part]
    early = [n for n in range(len(pieces)) if n not in late]
    total = pl.pallas_call(
        functools.partial(main_kernel, grid, width, blocks, len(pieces)),
        in_specs=[SMEM] + [VMEM] * (1 + len(early)),
        out_specs=VMEM,
        out_shape=pltpu.VMEM((rows, LANES), jnp.float32),
        scratch_shapes=[pltpu.VMEM((row_words + WORDS, lanes), jnp.float32)],
        compiler_params=PARAMS,
        cost_estimate=cost(2 * rows * row_words * PLANES * LANES, 4 * rows * row_words),
        name="mean_main",
    )(spot, here(short), *[here(pieces[n]) for n in early])
    late_cols = late_words.shape[1]
    half = rows // 2
    args = (spot, here(late_words), here(degree), here(total), here(own), *[here(pieces[n]) for n in late])

    def late_call(first_row):
        return pl.pallas_call(
            functools.partial(late_kernel, width, blocks, first_row),
            in_specs=[SMEM] + [VMEM] * (4 + len(late)),
            out_specs=VMEM,
            out_shape=pltpu.VMEM((width, half), jnp.bfloat16),
            scratch_shapes=[
                pltpu.VMEM((late_cols + WORDS, lanes), jnp.float32),
                pltpu.VMEM((half, late_cols), jnp.int16),
                pltpu.VMEM((half, LANES), jnp.float32),
            ],
            compiler_params=PARAMS,
            cost_estimate=cost(2 * half * late_cols * PLANES * LANES, 4 * half * LANES),
            name="mean_late",
        )(*args)

    return [late_call(0), late_call(half)]


def picked_by(values, at):
    chosen = values[0]
    for n in range(1, len(values)):
        chosen = jnp.where(at == n, values[n], chosen)
    return chosen


def hidden_kernel(width, classes, spare, blocks, grid, place_ref, *rest):
    _, _, n_col, n_batch = grid
    n_parts = 2 * n_col
    parts, packs = rest[:n_parts], rest[n_parts : n_parts + n_col * n_batch]
    hidden_ref, wide_ref, own_weight_ref, rows_ref, tall_ref, scratch_ref = rest[n_parts + n_col * n_batch :]
    col_at, batch_at = place_ref[1], place_ref[2]
    words = parts[0].shape[0]

    def weights(back, owner, low, count):
        found = [packs[back * n_batch + k][low : low + count, :] for k in range(n_batch)]
        return picked_by(found, behind(batch_at, owner, n_batch))

    first = [
        jnp.concatenate([weights(back, owner, half * width, width) for owner in range(n_batch)], axis=1)
        for half in range(2)
        for back in range(n_col)
    ]

    def class_weights(low):
        by_back = [weights(back, col_at, low, spare) for back in range(n_col)]
        return jnp.concatenate(
            [picked_by(by_back, behind(col_at, owner, n_col)) for owner in range(n_col)], axis=1
        )

    own_weight_ref[...] = class_weights(2 * width)
    far_weight = class_weights(2 * width + spare)
    for i in range(BITS):
        for n, part in enumerate(parts):
            rows_ref[pl.ds(i * words, words), n * width : (n + 1) * width] = part[:, i * width : (i + 1) * width]
    hidden = jnp.dot(rows_ref[...], jnp.concatenate(first, axis=0), preferred_element_type=jnp.float32)
    hidden = jnp.maximum(hidden, 0.0).astype(jnp.bfloat16)
    hidden_ref[...] = hidden
    tall_ref[...] = lax.dot_general(
        hidden, far_weight, (((1,), (1,)), ((), ())), preferred_element_type=jnp.float32
    )
    scratch_ref[...] = jnp.zeros_like(scratch_ref)
    for i in range(PLANES):
        scratch_ref[:, i * classes : (i + 1) * classes] = tall_ref[pl.ds(i * words, words), :classes]
    tiles, left = tiles_for(classes, blocks)
    for k in range(blocks):
        for t in range(tiles):
            wide_ref[k * tiles + t] = scratch_ref[
                k * WORDS : (k + 1) * WORDS, t * LANES : (t + 1) * LANES
            ].astype(jnp.bfloat16)
    if left:
        step = LANES // blocks
        lane = lax.broadcasted_iota(jnp.int32, (WORDS, LANES), 1)
        shared = jnp.zeros((WORDS, LANES), jnp.float32)
        for k in range(blocks):
            piece = scratch_ref[k * WORDS : (k + 1) * WORDS, tiles * LANES : (tiles + 1) * LANES]
            turned = pltpu.roll(piece, k * step, 1) if k else piece
            shared = jnp.where((lane >= k * step) & (lane < (k + 1) * step), turned, shared)
        wide_ref[blocks * tiles] = shared.astype(jnp.bfloat16)


def own_kernel(seed_ref, weight_ref, *rest):
    hidden_refs, out_ref = rest[:-1], rest[-1]
    total = jnp.zeros((weight_ref.shape[0], out_ref.shape[1]), jnp.float32)
    for n, hidden_ref in enumerate(hidden_refs):
        rows = hidden_ref.shape[0]
        every = lax.dot_general(
            weight_ref[...], hidden_ref[...], (((1,), (1,)), ((), ())), preferred_element_type=jnp.float32
        )
        high = every.astype(jnp.bfloat16)
        low = (every - high.astype(jnp.float32)).astype(jnp.bfloat16)
        place = lax.broadcasted_iota(jnp.int32, (rows, seed_ref.shape[1]), 0) + n * rows
        chosen = jnp.where(place == seed_ref[...], 1.0, 0.0).astype(jnp.bfloat16)
        total += jnp.dot(high, chosen, preferred_element_type=jnp.float32)
        total += jnp.dot(low, chosen, preferred_element_type=jnp.float32)
    out_ref[...] = jnp.zeros_like(out_ref)
    out_ref[: total.shape[0], :] = total


def per_device(
    grid,
    features,
    self_weight1,
    neigh_weight1,
    need_first,
    count_first,
    adjacency_first,
    self_weight2,
    neigh_weight2,
    need_second,
    count_second,
    adjacency_second,
    seed_rows,
):
    _, _, n_col, n_batch = grid
    dom_at, col_at, batch_at = (lax.axis_index(a) for a in MESH_AXES)

    def move(array, which, by):
        return lax.ppermute(array, MESH_AXES, shift_perm(grid, which, by))

    def ring(array, which):
        return [array] + [move(array, which, by) for by in range(1, grid[which])]

    def gather_blocks(piece):
        return [last for first in ring(piece, 0) for second in ring(first, 1) for last in ring(second, 3)]

    def in_order(relative, at):
        n = len(relative)
        ordered = []
        for owner in range(n):
            chosen = relative[0]
            for back in range(1, n):
                chosen = jnp.where(behind(at, owner, n) == back, relative[back], chosen)
            ordered.append(chosen)
        return ordered

    width = features.shape[1]
    rows = adjacency_first.shape[0]
    words = rows // BITS
    blocks = rows // BLK

    place = jnp.stack([dom_at, col_at, batch_at])
    prepared = prepare_call(grid, place, need_second[0], count_second, adjacency_second, blocks)

    own = lax.dynamic_slice_in_dim(features, batch_at * rows, rows, 0).reshape(words, BITS * width)
    tiles = tiles_for(width, blocks)[0]
    sent = own[:, : tiles * LANES].reshape(blocks, WORDS, tiles, LANES).transpose(0, 2, 1, 3)
    pieces_first = gather_blocks(sent.reshape(blocks * tiles, WORDS, LANES))

    self_parts = ring(own, 2)
    class_cols = self_weight2.shape[1]
    classes = class_cols * n_batch // n_col
    spare = -(-class_cols // 16) * 16
    tall2 = [jnp.pad(w.T, ((0, spare - class_cols), (0, 0))) for w in (self_weight2, neigh_weight2)]
    packed = jnp.concatenate([self_weight1, neigh_weight1, *tall2], axis=0)
    packs = [p for a in ring(packed, 2) for p in ring(a, 3)]

    near = mean_call(grid, place, need_first[0], count_first, adjacency_first, pieces_first, blocks, width)
    near_parts = ring(near, 2)
    wide = lanes_for(classes)
    tiles, left = tiles_for(classes, blocks)
    hidden_cols = self_weight1.shape[1] * n_batch
    hidden, scores, weight_own = pl.pallas_call(
        functools.partial(hidden_kernel, width, classes, spare, blocks, grid),
        in_specs=[SMEM] + [VMEM] * (2 * n_col + n_col * n_batch),
        out_specs=[VMEM] * 3,
        out_shape=[
            pltpu.VMEM((rows, hidden_cols), jnp.bfloat16),
            pltpu.VMEM((blocks * tiles + (left > 0), WORDS, LANES), jnp.bfloat16),
            pltpu.VMEM((spare, hidden_cols), jnp.bfloat16),
        ],
        scratch_shapes=[
            pltpu.VMEM((rows, 2 * n_col * width), jnp.bfloat16),
            pltpu.VMEM((rows, spare), jnp.float32),
            pltpu.VMEM((words, wide), jnp.float32),
        ],
        compiler_params=PARAMS,
        name="hidden",
    )(place, *[here(a) for a in (*self_parts, *near_parts, *packs)])

    pieces_second = gather_blocks(scores)
    inside = seed_rows % rows
    seed_at = behind(batch_at, seed_rows // rows, n_batch) * rows + (inside % BITS) * words + inside // BITS
    seeds = seed_rows.shape[0]
    own_call = pl.pallas_call(
        own_kernel,
        in_specs=[VMEM] * (2 + n_batch),
        out_specs=VMEM,
        out_shape=pltpu.VMEM((LANES, seeds), jnp.float32),
        compiler_params=PARAMS,
        cost_estimate=pl.CostEstimate(
            flops=12 * rows * n_batch * seeds * LANES, bytes_accessed=4 * classes * seeds, transcendentals=0
        ),
        name="own_rows",
    )
    hidden_parts = ring(hidden, 3)
    own_second = own_call(seed_at.reshape(1, seeds), here(weight_own), *[here(h) for h in hidden_parts])
    halves = split_mean_calls(grid, prepared, pieces_second, own_second, blocks, classes)
    halves = [jnp.concatenate(in_order(ring(h, 2), col_at), axis=0) for h in halves]
    return jnp.concatenate(halves, axis=1).astype(jnp.float32).T


def solution(mesh):
    sizes = tuple(mesh.shape[a] for a in MESH_AXES)
    inner = 2 if sizes[0] % 2 == 0 else 1
    grid = (sizes[0] // inner, inner, sizes[1], sizes[2])
    placed = (
        P("dom", "col"),
        P("col", "batch"),
        P("col", "batch"),
        P(("dom", "batch"), None),
        P(("dom", "batch")),
        P(("dom", "batch"), None),
        P("col", "batch"),
        P("col", "batch"),
        P(("dom", "batch"), None),
        P(("dom", "batch")),
        P(("dom", "batch"), None),
        P(("dom", "batch")),
    )

    def body(*args):
        return per_device(grid, *args)

    return jax.shard_map(
        body, mesh=mesh, in_specs=placed, out_specs=P(("dom", "batch"), None), check_vma=False
    )
```
